32 devices in a mesh: gx: 4 (over z), gy: 8 (over y, x, core).
Axes of the slice: x: 2, y: 2, z: 4, core: 2. Of those that a mesh axis runs over, the one named last changes fastest.
Arguments:
- rhs: float32 [4, 128, 16384], P(None, None, ('gx', 'gy')), may hold values from -6 to 6
- offsets: float32 [3, 128, 16384], P(None, None, ('gx', 'gy')), may hold values from -4 to 4
- lengths: float32 [16384], P(('gx', 'gy')), may hold values from 1 to 4
- bucket: int32 [16384, 1], P(('gx', 'gy')), may hold values from 0 to 3; in each aligned block of 512 rows (0 to 511, 512 to 1023, ...) at most 128 rows name the same one
- attach: int32 [16384], P(('gx', 'gy')), may hold values from 0 to 511
- operator: float32 [4, 512, 512], P('gx'), may hold values from -0.25 to 0.25
- inverse: float32 [4, 512, 512], P('gx'), as said below
- mobility: float32 [36, 2048], P(None, ('gx', 'gy')), may hold values from -2.5 to 2.5
Outputs:
- velocity: float32 [4, 128, 16384], P(None, None, ('gx', 'gy'))
The draws below stay inside these ranges and needn't reach their ends.
Inputs may be any that keep to these rules, and one draw needn't show every extreme that they name: Bucket b owns fibers of 16 * 2^(b mod 4) nodes. Among the 512 fibers of one device no bucket has more than 128, and in every draw some bucket has exactly 128 there. `inverse`: identity plus a dense full-rank part.
All inputs are finite; a program needn't handle non-finite values.
Results may differ from the reference program's by a relative error of at most 0.0003.
Values sent between devices are 32-bit elements; how exact they have to be, the bound alone decides.
No kernel may reach another device: no remote copies, remote signals or barrier semaphores. Data moves between devices by JAX's collectives and lax.ppermute only.
A program may use at most 64 MiB of HBM per device.

```python
import math
import jax
import jax.numpy as jnp
import numpy as np
from jax import lax

NODE_MIN = 16
NODE_MAX = 128
ITERS = 4
FIB_DEV = 512
CEN_DEV = 64
CEN_SLAB = 512
FIBERS = 16384
CENTROS = 2048
N_GX = 4
N_GY = 8


def draw_inverse(key, part):
    order_size = 4 * NODE_MAX
    noise = jax.random.normal(key, (N_GX, order_size, order_size), jnp.float32)
    return jnp.eye(order_size, dtype=jnp.float32)[None] + 0.4 * noise / math.sqrt(order_size)


def set_ends(drawn, key, smallest, largest):
    place = [jax.random.randint(jax.random.fold_in(key, axis), (), 0, length) for axis, length in enumerate(drawn.shape)]
    longest = drawn.shape.index(max(drawn.shape))
    next_to = place[:longest] + [(place[longest] + 1) % drawn.shape[longest]] + place[longest + 1:]
    return drawn.at[tuple(place)].set(smallest).at[tuple(next_to)].set(largest)


def block_levels(own_key, shape, shards, low, largest):
    factor_of = 1.0
    for dim, parts in shards:
        steps = jax.random.uniform(jax.random.fold_in(jax.random.fold_in(own_key, 6), dim), (parts,), jnp.float32, low / len(shards), largest / len(shards))
        factor_of = factor_of * jnp.repeat(jnp.exp(steps), shape[dim] // parts).reshape((-1,) + (1,) * (len(shape) - 1 - dim))
    return factor_of


def deal_out(own_key, own, number, rows, count, top, most, slope):
    ranking = jax.random.permutation(own_key, count)
    heavy_load, common = shares(count, rows * top, most, slope, True), shares(count, rows * top, most, slope, False)
    places = jnp.arange(count)

    def named(sizes, offset_by):
        used = int((sizes > 0).sum())
        fixed = max(1, used // 4)
        moved = fixed + (places - fixed + offset_by * (used - fixed)) % max(1, count - fixed)
        return jnp.zeros((count,), jnp.int32).at[ranking[jnp.where(places < fixed, places, moved)]].set(jnp.asarray(sizes, jnp.int32))

    sizes = jnp.where(number % 4 == 0, named(heavy_load, number // 4), named(common, number - number // 4 - 1))
    mixed = jax.random.permutation(jax.random.fold_in(own, 3), count)
    source_of, sink = mixed[0:count // 2 * 2:2], mixed[1:count // 2 * 2:2]
    slack = jnp.minimum(sizes[source_of] - 1, most - sizes[sink]) // 2
    slack = jnp.where((source_of == ranking[0]) | (sink == ranking[0]) | (sizes[sink] == 0), 0, jnp.maximum(slack, 0))
    moved = jax.random.randint(jax.random.fold_in(own, 4), (count // 2,), 0, 1 << 20) % (slack + 1)
    sizes = sizes.at[source_of].add(-moved).at[sink].add(moved)
    members = jnp.searchsorted(jnp.cumsum(sizes), jnp.arange(rows * top), side="right").astype(jnp.int32)
    listing = members.reshape(top, rows).T
    listing = listing[jax.random.permutation(jax.random.fold_in(own, 1), rows)]
    offset_by = jax.random.randint(jax.random.fold_in(own, 2), (rows, 1), 0, top)
    return jnp.take_along_axis(listing, (jnp.arange(top)[None, :] + offset_by) % top, axis=1)


def shares(amount, total, bound, lean, full):
    portions = [(1 << 20) // math.isqrt(grade ** lean) + 1 for grade in range(1, amount + 1)]
    largest = bound if full else min(bound, max(-(-total // amount), total * portions[0] // sum(portions)))
    least = 1 if total - largest >= amount - 1 else 0
    holding, spare = [largest] + [least] * (amount - 1), total - largest - least * (amount - 1)
    while spare > 0:
        free = [i for i in range(1, amount) if holding[i] < largest] or [i for i in range(1, amount) if holding[i] < bound]
        pool, left = sum([portions[i] for i in free]), spare
        for i in free:
            addition = min(bound - holding[i], max(1, left * portions[i] // pool), spare)
            holding[i] = holding[i] + addition
            spare = spare - addition
    return np.array(holding)


def gaussian(stream_key, dims, deviation, limit, split=(), kind=jnp.bfloat16):
    loudness = block_levels(stream_key, dims, split, -0.22, 0.18) if split else 1.0
    drawn = jax.random.normal(stream_key, dims, jnp.float32) * deviation * loudness
    return jnp.minimum(jnp.maximum(drawn, -limit), limit).astype(kind)


def setup_inputs(seed: int = 0) -> dict:
    splits = jax.random.split(jax.random.key(seed), 9)
    rhs = gaussian(splits[0], (4, NODE_MAX, FIBERS), 1.0, 6.0, ((2, 32),), jnp.float32)
    offsets = gaussian(splits[1], (3, NODE_MAX, FIBERS), 0.6, 4.0, ((2, 32),), jnp.float32)
    lengths = jnp.clip(jnp.exp(math.log(4.0) - 1.3862944 * jax.random.uniform(splits[2], (FIBERS,), jnp.float32) ** block_levels(splits[2], (FIBERS,), ((0, 32),), -0.2, 0.2)), 1.0, 4.0)
    bucket_keys = jax.random.split(jax.random.fold_in(splits[3], 1), FIBERS // FIB_DEV)
    bucket_turns = jax.random.permutation(jax.random.fold_in(splits[3], 3), FIBERS // FIB_DEV)
    bucket = jax.vmap(lambda own, number: deal_out(jax.random.fold_in(splits[3], 2), own, number, FIB_DEV, N_GX, 1, FIB_DEV // 4, 2))(bucket_keys, bucket_turns).reshape((FIBERS, 1))
    attach = set_ends(jax.random.randint(splits[4], (FIBERS,), 0, CEN_SLAB), jax.random.fold_in(splits[4], 1), 0, CEN_SLAB - 1).astype(jnp.int32)
    operator = gaussian(splits[5], (N_GX, 4 * NODE_MAX, 4 * NODE_MAX), (4 * NODE_MAX) ** -0.5, 0.25, ((0, 4),), jnp.float32)
    inverse = draw_inverse(jax.random.fold_in(splits[8], 71), 0)
    mobility = gaussian(splits[7], (36, CENTROS), 6 ** -0.5, 2.5, ((1, 32),), jnp.float32)
    return {"rhs": rhs, "offsets": offsets, "lengths": lengths, "bucket": bucket, "attach": attach, "operator": operator, "inverse": inverse, "mobility": mobility}


PRECISE = lax.Precision.HIGHEST


def couple(geometry, iterate):
    along = jnp.sum(geometry * iterate[:3], axis=0)
    transverse = geometry * (along + iterate[3])[None]
    return 0.15 * jnp.concatenate([transverse, along[None]], axis=0)


def reference(rhs, offsets, lengths, bucket, attach, operator, inverse, mobility):
    fibers = rhs.shape[2]
    nodes_max = rhs.shape[1]
    target = bucket[:, 0].astype(jnp.int32)
    levels = target % 4
    counts = NODE_MIN * jnp.left_shift(jnp.ones_like(levels), levels)
    fiber_index = jnp.arange(fibers, dtype=jnp.int32)
    node_mask = (jnp.arange(nodes_max, dtype=jnp.int32)[:, None] < counts[None, :]).astype(jnp.float32)
    geometry = offsets * node_mask
    coefficient = 0.3 / lengths
    capacity = (FIB_DEV // 4) * N_GX * N_GY
    solution = jnp.zeros((4, nodes_max, fibers), jnp.float32)
    for bucket_id in range(N_GX):
        node_count = NODE_MIN * 2 ** (bucket_id % 4)
        order_size = 4 * node_count
        chosen = target == bucket_id
        position = jnp.cumsum(chosen.astype(jnp.int32)) - 1
        position = jnp.where(chosen, position, capacity).astype(jnp.int32)
        slot_fiber = jnp.full((capacity,), fibers, jnp.int32).at[position].set(fiber_index, mode="drop")
        live_slot = (slot_fiber < fibers).astype(jnp.float32)
        picked = jnp.minimum(slot_fiber, fibers - 1).astype(jnp.int32)
        source = rhs[:, :node_count][:, :, picked] * live_slot
        geometry_b = geometry[:, :node_count][:, :, picked]
        factor = coefficient[picked] * live_slot
        stiffness = operator[bucket_id].reshape(4, nodes_max, 4, nodes_max)[:, :node_count, :, :node_count].reshape(order_size, order_size)
        inverse_b = inverse[bucket_id].reshape(4, nodes_max, 4, nodes_max)[:, :node_count, :, :node_count].reshape(order_size, order_size)

        def multiply(matrix, vector):
            product = jnp.dot(matrix, vector.reshape(order_size, capacity), precision=PRECISE)
            return product.reshape(4, node_count, capacity)

        iterate = multiply(inverse_b, source)
        for sweep in range(ITERS):
            iterate = multiply(inverse_b, source - factor * multiply(stiffness, iterate) - couple(geometry_b, iterate))
        solution = solution.at[:, :node_count, slot_fiber].set(iterate, mode="drop")
    weight = lengths / counts.astype(jnp.float32)
    clamp_force = weight * jnp.sum(solution[:3], axis=1)
    torque = weight * jnp.sum(jnp.cross(geometry, solution[:3], axis=0), axis=1)
    wrench = jnp.concatenate([clamp_force, torque], axis=0)
    slab_index = fiber_index // (FIB_DEV * N_GY)
    centre = (slab_index * (CEN_DEV * N_GY) + attach).astype(jnp.int32)
    wrench_table = jnp.zeros((6, CEN_DEV * N_GY * N_GX), jnp.float32).at[:, centre].add(wrench)
    motion = jnp.sum(mobility.reshape(6, 6, -1) * wrench_table[None], axis=1)
    moving = motion[:, centre]
    rigid_motion = moving[:3, None, :] + jnp.cross(moving[3:, None, :], geometry, axis=0)
    return jnp.concatenate([solution[:3] + rigid_motion * node_mask[None], solution[3:]], axis=0)
```

```python
import jax
import jax.numpy as jnp
from jax import lax
from jax.experimental import pallas as pl
from jax.experimental.pallas import tpu as pltpu
from jax.sharding import PartitionSpec as P


NODE_MIN = 16
LEVELS = 4
ITERS = 4
SLOT_CAP = 128
VMEM_LIMIT = 32 << 20
F32 = jnp.float32
BF16 = jnp.bfloat16
NN = (((1,), (0,)), ((), ()))
NT = (((1,), (1,)), ((), ()))


def split(value):
    high = value.astype(BF16)
    low = (value - high.astype(F32)).astype(BF16)
    return high, low


def mm(a, b, dims=NN):
    return lax.dot_general(a, b, dims, preferred_element_type=F32)


def pick(value, onehot, dims):
    high, low = split(value)
    return mm(high, onehot, dims) + mm(low, onehot, dims)


VM = pl.BlockSpec(memory_space=pltpu.VMEM)
ANY = pl.BlockSpec(memory_space=pl.ANY)


def near(*values):
    return tuple(pltpu.with_memory_space_constraint(v, pltpu.VMEM) for v in values)


def call(kernel, outs, far=(), values=(), scratch=(), far_out=False, flops=0):
    if far_out:
        out_shape = tuple(jax.ShapeDtypeStruct(shape, kind) for shape, kind in outs)
    else:
        out_shape = tuple(pltpu.VMEM(shape, kind) for shape, kind in outs)
    return pl.pallas_call(
        kernel,
        out_shape=out_shape,
        in_specs=[ANY] * len(far) + [VM] * len(values),
        out_specs=tuple(ANY if far_out else VM for _ in outs),
        scratch_shapes=list(scratch),
        compiler_params=pltpu.CompilerParams(vmem_limit_bytes=VMEM_LIMIT),
        cost_estimate=pl.CostEstimate(flops=flops, transcendentals=0, bytes_accessed=1 << 20),
    )(*far, *near(*values))


def take_share(operator, inverse, rows):
    width = operator.shape[1]

    def kernel(op_ref, inv_ref, a_ref, sem):
        seat = lax.axis_index("gy")

        def load(src):
            copy = pltpu.make_async_copy(src.at[pl.ds((seat // 2) * rows, rows)], a_ref, sem)
            copy.start()
            copy.wait()

        @pl.when(seat % 2 == 0)
        def _():
            load(inv_ref)

        @pl.when(seat % 2 != 0)
        def _():
            load(op_ref)

    return call(
        kernel,
        [((rows, width), F32)],
        far=(operator, inverse),
        scratch=[pltpu.SemaphoreType.DMA],
        flops=1 << 20,
    )[0]


def pack_blocks(operator, inverse, mobility, nodes):
    half, quarter = nodes // 2, nodes // 4
    entries, seat_lanes = mobility.shape
    groups = -(-entries // 8)
    assert 2 * seat_lanes == nodes and groups <= 8

    def kernel(op_ref, inv_ref, mob_ref, mid_ref, small_ref, ext_ref, buf, sems):
        seat = lax.axis_index("gy")
        level = lax.axis_index("gx") % LEVELS

        def load(src):
            copies = [
                pltpu.make_async_copy(
                    src.at[pl.ds(c * nodes, half)], buf.at[pl.ds(c * half, half)], sems.at[c]
                )
                for c in range(4)
            ]
            for copy in copies:
                copy.start()
            for copy in copies:
                copy.wait()

        @pl.when(seat % 2 == 0)
        def _():
            load(inv_ref)

        @pl.when(seat % 2 != 0)
        def _():
            load(op_ref)

        lane = lax.broadcasted_iota(jnp.int32, (4 * half, nodes), 1)
        for pair in range(2):
            first = buf[:, pl.ds(2 * pair * nodes, nodes)]
            second = pltpu.roll(buf[:, pl.ds((2 * pair + 1) * nodes, nodes)], half, 1)
            mid_ref[:, pl.ds(pair * nodes, nodes)] = jnp.where(lane < half, first, second)
        count = jnp.left_shift(jnp.int32(NODE_MIN), level)
        lane = lax.broadcasted_iota(jnp.int32, (quarter, nodes), 1)
        row = lax.broadcasted_iota(jnp.int32, (quarter, nodes), 0)
        keep = ((lane % quarter) < count) & (row < count)
        for c in range(4):
            block = jnp.zeros((quarter, nodes), F32)
            for d in range(4):
                part = buf[pl.ds(c * half, quarter), pl.ds(d * nodes, nodes)]
                if d:
                    part = pltpu.roll(part, d * quarter, 1)
                block = jnp.where(lane // quarter == d, part, block)
            small_ref[pl.ds(c * quarter, quarter), :] = jnp.where(keep, block, 0.0)
        parts = []
        for g in range(8):
            size = max(0, min(8, entries - 8 * g))
            part = jnp.zeros((8, seat_lanes), F32)
            if size:
                part = mob_ref[pl.ds(8 * g, size), :]
                if size < 8:
                    part = jnp.concatenate([part, jnp.zeros((8 - size, seat_lanes), F32)], axis=0)
            parts.append(part)
        ext_ref[...] = jnp.concatenate(parts, axis=1)

    return call(
        kernel,
        [
            ((4 * half, 4 * half), F32),
            ((4 * quarter, 4 * quarter), F32),
            ((8, 8 * seat_lanes), F32),
        ],
        far=(operator, inverse),
        values=(mobility,),
        scratch=[pltpu.VMEM((4 * half, 4 * nodes), F32), pltpu.SemaphoreType.DMA((4,))],
        flops=1 << 20,
    )


def grade(buckets):
    small = [b for b in range(buckets) if b % LEVELS < LEVELS - 2]
    mid = [b for b in range(buckets) if b % LEVELS == LEVELS - 2]
    top = [b for b in range(buckets) if b % LEVELS == LEVELS - 1]
    return small, mid, top


def sort_fibers(bucket, attach, lengths, rhs, offsets, buckets, centres, nodes):
    fibers = bucket.shape[1]
    groups = grade(buckets)
    order = [b for group in groups for b in group]
    spans = [nodes // 4, nodes // 2, nodes]

    def kernel(bk_ref, at_ref, len_ref, rhs_ref, off_ref, oh_ref, s_ref, *rest):
        sorted_refs, aux_ref = rest[:3], rest[3]
        bk = bk_ref[...]
        ids = lax.broadcasted_iota(jnp.int32, (max(8, buckets), fibers), 0)
        mark = (ids == bk).astype(BF16)
        upper = (
            lax.broadcasted_iota(jnp.int32, (fibers, fibers), 0)
            < lax.broadcasted_iota(jnp.int32, (fibers, fibers), 1)
        ).astype(BF16)
        before = mm(mark, upper)
        place = jnp.sum(jnp.where(ids == bk, before, 0.0), axis=0, keepdims=True).astype(jnp.int32)
        slot = lax.broadcasted_iota(jnp.int32, (SLOT_CAP, fibers), 0)
        for k, b in enumerate(order):
            hot = (slot == place) & (bk == b)
            oh_ref[pl.ds(k * SLOT_CAP, SLOT_CAP), :] = hot.astype(BF16)
        onehot = oh_ref[...]
        centre = (
            lax.broadcasted_iota(jnp.int32, (centres, fibers), 0) == at_ref[...]
        ).astype(BF16)
        s_ref[...] = mm(onehot, centre, NT).astype(BF16)
        length = len_ref[...]
        row = lax.broadcasted_iota(jnp.int32, (8, fibers), 0)
        aux = jnp.where(row == 0, 0.3 / length, jnp.where(row == 1, length, 0.0))
        aux_ref[...] = pick(aux, onehot, NT)
        start = 0
        for group, span, ref in zip(groups, spans, sorted_refs):
            hot = oh_ref[pl.ds(start, len(group) * SLOT_CAP), :]
            start += len(group) * SLOT_CAP
            for c in range(7):
                src = rhs_ref[c, pl.ds(0, span), :] if c < 4 else off_ref[c - 4, pl.ds(0, span), :]
                ref[pl.ds(c * span, span), :] = pick(src, hot, NT)

    return call(
        kernel,
        [
            ((buckets * SLOT_CAP, fibers), BF16),
            ((buckets * SLOT_CAP, centres), BF16),
            *[
                ((7 * span, len(group) * SLOT_CAP), F32)
                for group, span in zip(groups, spans)
            ],
            ((8, buckets * SLOT_CAP), F32),
        ],
        values=(bucket, attach, lengths, rhs, offsets),
        flops=1 << 30,
    )


def product(matrix, vector):
    high, low = matrix
    v_high, v_low = split(vector)
    width = vector.shape[1]
    both = mm(high, jnp.concatenate([v_high, v_low], axis=1))
    return both[:, :width] + both[:, width:] + mm(low, v_high)


def couple(geometry, vector, n):
    u = [vector[c * n:(c + 1) * n] for c in range(4)]
    o = [geometry[c * n:(c + 1) * n] for c in range(3)]
    along = o[0] * u[0] + o[1] * u[1] + o[2] * u[2]
    pull = along + u[3]
    return 0.15 * jnp.concatenate([o[0] * pull, o[1] * pull, o[2] * pull, along], axis=0)


def sweeps(systems):
    vectors = [product(inverse, source) for inverse, _, source, _, _, _ in systems]
    for _ in range(ITERS):
        forces = [
            source - factor * product(stiffness, v) - couple(geometry, v, n)
            for v, (_, stiffness, source, geometry, factor, n) in zip(vectors, systems)
        ]
        vectors = [product(system[0], force) for force, system in zip(forces, systems)]
    return vectors


def wrench_rows(vector, geometry, length, n, count):
    u = [vector[c * n:(c + 1) * n] for c in range(3)]
    o = [geometry[c * n:(c + 1) * n] for c in range(3)]
    sums = [jnp.sum(v, axis=0, keepdims=True) for v in u]
    for a, b in ((1, 2), (2, 0), (0, 1)):
        sums.append(jnp.sum(o[a] * u[b] - o[b] * u[a], axis=0, keepdims=True))
    zero = jnp.zeros_like(sums[0])
    return (length / count) * jnp.concatenate(sums + [zero, zero], axis=0)


def solve_low(smalls, mids, sorted_small, sorted_mid, aux, slots, buckets, nodes):
    small, mid, _ = grade(buckets)
    centres = slots.shape[1]
    half, quarter = nodes // 2, nodes // 4

    def kernel(so_ref, st_ref, mo_ref, mt_ref, ss_ref, sm_ref, aux_ref, slot_ref, xs_ref, xm_ref, t_ref):
        gx = lax.axis_index("gx")
        first = lax.axis_index("gy") % 2 == 0
        systems, lengths, counts = [], [], []
        for k, b in enumerate(small + mid):
            lanes = pl.ds(k * SLOT_CAP, SLOT_CAP)
            if k < len(small):
                index = lax.rem(b - gx + buckets, buckets)
                mine, theirs, ref, here, n = so_ref[index], st_ref[index], ss_ref, lanes, quarter
            else:
                j = k - len(small)
                here = pl.ds(j * SLOT_CAP, SLOT_CAP)
                mine, theirs, ref, n = mo_ref[j], mt_ref[j], sm_ref, half
            systems.append(
                (
                    split(jnp.where(first, mine, theirs)),
                    split(jnp.where(first, theirs, mine)),
                    ref[pl.ds(0, 4 * n), here],
                    ref[pl.ds(4 * n, 3 * n), here],
                    aux_ref[pl.ds(0, 1), lanes],
                    n,
                )
            )
            lengths.append(aux_ref[pl.ds(1, 1), lanes])
            counts.append(float(NODE_MIN * 2 ** (b % LEVELS)))
        vectors = sweeps(systems)
        table = jnp.zeros((8, centres), F32)
        for k, vector in enumerate(vectors):
            _, _, _, geometry, _, n = systems[k]
            rows = wrench_rows(vector, geometry, lengths[k], n, counts[k])
            table = table + pick(rows, slot_ref[pl.ds(k * SLOT_CAP, SLOT_CAP), :], NN)
            if k < len(small):
                xs_ref[:, pl.ds(k * SLOT_CAP, SLOT_CAP)] = vector
            else:
                xm_ref[:, pl.ds((k - len(small)) * SLOT_CAP, SLOT_CAP)] = vector
        t_ref[...] = table

    return call(
        kernel,
        [
            ((4 * quarter, len(small) * SLOT_CAP), F32),
            ((4 * half, len(mid) * SLOT_CAP), F32),
            ((8, centres), F32),
        ],
        values=(*smalls, *mids, sorted_small, sorted_mid, aux, slots),
        flops=1 << 30,
    )


def solve_top(pieces, top, aux, slots, table, buckets, nodes, rows):
    _, _, names = grade(buckets)
    n_low = buckets - len(names)
    width = LEVELS * nodes
    centres = slots.shape[1]
    shares = width // rows
    flat = [p for pair in pieces for side in pair for p in side]

    def kernel(*refs):
        piece_refs = refs[:len(flat)]
        top_ref, aux_ref, slot_ref, tin_ref, x_ref, t_ref, high, low = refs[len(flat):]
        seat = lax.axis_index("gy")
        chip, core = seat // 2, seat % 2
        total = tin_ref[...]
        for k in range(len(names)):
            for side in range(2):
                matrix = core if side == 0 else 1 - core
                for m in range(shares):
                    ref = piece_refs[(k * 2 + side) * shares + m]
                    h, l = split(ref[pl.ds(0, rows), :])
                    place = pl.ds(pl.multiple_of(jnp.bitwise_xor(chip, m) * rows, rows), rows)
                    high[matrix, place, :] = h
                    low[matrix, place, :] = l
            lanes = pl.ds(k * SLOT_CAP, SLOT_CAP)
            aux_lanes = pl.ds((n_low + k) * SLOT_CAP, SLOT_CAP)
            source = top_ref[pl.ds(0, width), lanes]
            geometry = top_ref[pl.ds(width, 3 * nodes), lanes]
            factor = aux_ref[pl.ds(0, 1), aux_lanes]
            length = aux_ref[pl.ds(1, 1), aux_lanes]
            (vector,) = sweeps(
                [((high[0], low[0]), (high[1], low[1]), source, geometry, factor, nodes)]
            )
            x_ref[:, lanes] = vector
            out = wrench_rows(vector, geometry, length, nodes, float(nodes))
            total = total + pick(out, slot_ref[aux_lanes, :], NN)
        t_ref[...] = total

    return call(
        kernel,
        [((width, len(names) * SLOT_CAP), F32), ((8, centres), F32)],
        values=(*flat, top, aux, slots, table),
        scratch=[
            pltpu.VMEM((2, width, width), BF16),
            pltpu.VMEM((2, width, width), BF16),
        ],
        flops=1 << 31,
    )


def unsort(parts, onehot, pieces, nodes, rows):
    fibers = onehot.shape[1]
    spans = [nodes // 4, nodes // 2, nodes]
    own, other = pieces
    chips = len(own)

    def kernel(*refs):
        part_refs, oh_ref = refs[:3], refs[3]
        own_refs, other_refs = refs[4:4 + chips], refs[4 + chips:4 + 2 * chips]
        out_ref, mob_ref = refs[4 + 2 * chips:]
        for c in range(4):
            total, start = None, 0
            for ref, span in zip(part_refs, spans):
                hot = oh_ref[pl.ds(start, ref.shape[1]), :]
                start += ref.shape[1]
                value = pick(ref[pl.ds(c * span, span), :], hot, NN)
                if total is not None:
                    low = total.shape[0]
                    value = jnp.concatenate([value[:low] + total, value[low:]], axis=0)
                total = value
            out_ref[c] = total
        seat = lax.axis_index("gy")
        chip, even = seat // 2, seat % 2 == 0
        lane = lax.broadcasted_iota(jnp.int32, (8, nodes), 1)
        half = nodes // 2
        for m in range(chips):
            place = pl.ds(pl.multiple_of(jnp.bitwise_xor(chip, m) * nodes, nodes), nodes)
            for g in range(mob_ref.shape[0] // 8):
                tile = pl.ds((g // 2) * nodes, nodes)
                mine = own_refs[m][pl.ds(rows, 8), tile]
                theirs = other_refs[m][pl.ds(rows, 8), tile]
                first = jnp.where(even, mine, theirs)
                second = jnp.where(even, theirs, mine)
                if g % 2 == 0:
                    second = pltpu.roll(second, half, 1)
                else:
                    first = pltpu.roll(first, half, 1)
                mob_ref[pl.ds(8 * g, 8), place] = jnp.where(lane < half, first, second)

    return call(
        kernel,
        [((4, nodes, fibers), F32), ((40, chips * nodes), F32)],
        values=(*parts, onehot, *own, *other),
        flops=1 << 28,
    )


def finish(tables, mobility, bucket, attach, offsets, solved, nodes):
    fibers = bucket.shape[1]
    centres = mobility.shape[1]

    def kernel(*refs):
        t_refs = refs[:len(tables)]
        mob_ref, bk_ref, at_ref, off_ref, sol_ref, out_ref, buf, sems = refs[len(tables):]
        copies = [pltpu.make_async_copy(sol_ref.at[3], out_ref.at[3], sems.at[3])]
        copies[0].start()
        table = t_refs[0][...]
        for t in t_refs[1:]:
            table = table + t[...]
        rows = []
        for k in range(6):
            part = mob_ref[pl.ds(6 * k, 6), :] * table[:6]
            rows.append(jnp.sum(part, axis=0, keepdims=True))
        zero = jnp.zeros_like(rows[0])
        motion = jnp.concatenate(rows + [zero, zero], axis=0)
        centre = (
            lax.broadcasted_iota(jnp.int32, (centres, fibers), 0) == at_ref[...]
        ).astype(BF16)
        moving = pick(motion, centre, NN)
        counts = jnp.left_shift(jnp.int32(NODE_MIN), bk_ref[...] % LEVELS)
        mask = lax.broadcasted_iota(jnp.int32, (nodes, fibers), 0) < counts
        u = [moving[k:k + 1] for k in range(3)]
        w = [moving[3 + k:4 + k] for k in range(3)]
        for k, (a, b) in enumerate(((1, 2), (2, 0), (0, 1))):
            rigid = u[k] + (w[a] * off_ref[b] - w[b] * off_ref[a])
            buf[k] = sol_ref[k] + jnp.where(mask, rigid, 0.0)
            copy = pltpu.make_async_copy(buf.at[k], out_ref.at[k], sems.at[k])
            copy.start()
            copies.append(copy)
        for copy in copies:
            copy.wait()

    return call(
        kernel,
        [((4, nodes, fibers), F32)],
        values=(*tables, mobility, bucket, attach, offsets, solved),
        scratch=[pltpu.VMEM((3, nodes, fibers), F32), pltpu.SemaphoreType.DMA((4,))],
        far_out=True,
        flops=1 << 24,
    )[0]


def body(rhs, offsets, lengths, bucket, attach, operator, inverse, mobility):
    nodes, fibers = rhs.shape[1], rhs.shape[2]
    buckets = lax.axis_size("gx")
    seats = lax.axis_size("gy")
    chips = seats // 2
    rows = LEVELS * nodes // chips
    gx = lax.axis_index("gx")
    centres = mobility.shape[1] * seats
    small, mid, top = grade(buckets)

    def hop(value, m):
        return lax.ppermute(value, "gy", [(i, i ^ m) for i in range(seats)])

    def spread(value, source):
        mine = jnp.where(gx == source, value, 0.0)
        for target in range(buckets):
            if target != source:
                got = lax.ppermute(value, "gx", [(source, target)])
                mine = mine + got
        return mine

    share = take_share(operator[0], inverse[0], rows)
    shares = [spread(share, source) for source in top]
    block_mid, block_small, extra = pack_blocks(
        operator[0], inverse[0], mobility, nodes
    )
    shares[0] = jnp.concatenate([shares[0], extra], axis=0)
    mids = jnp.stack([spread(block_mid, source) for source in mid])
    smalls = [block_small]
    for shift in range(1, buckets):
        smalls.append(lax.ppermute(block_small, "gx", [(s, (s - shift) % buckets) for s in small]))
    smalls = jnp.stack(smalls)

    bucket_row = bucket.reshape(1, fibers)
    attach_row = attach.reshape(1, fibers)
    onehot, slots, sorted_small, sorted_mid, sorted_top, aux = sort_fibers(
        bucket_row, attach_row, lengths.reshape(1, fibers), rhs, offsets,
        buckets, centres, nodes,
    )

    pieces = []
    for mine in shares:
        own = [mine] + [hop(mine, 2 * m) for m in range(1, chips)]
        other = [hop(piece, 1) for piece in own]
        pieces.append((own, other))

    other_mids = hop(mids, 1)
    other_smalls = hop(smalls, 1)
    x_small, x_mid, table_low = solve_low(
        (smalls, other_smalls), (mids, other_mids), sorted_small, sorted_mid,
        aux, slots, buckets, nodes,
    )
    x_top, table = solve_top(pieces, sorted_top, aux, slots, table_low, buckets, nodes, rows)

    table = table + hop(table, 1)
    tables = [table] + [hop(table, 2 * m) for m in range(1, chips)]
    solved, mobility_all = unsort(
        (x_small, x_mid, x_top), onehot, pieces[0], nodes, rows
    )
    return finish(tables, mobility_all, bucket_row, attach_row, offsets, solved, nodes)


def solution(mesh):
    in_specs = (
        P(None, None, ("gx", "gy")),
        P(None, None, ("gx", "gy")),
        P(("gx", "gy")),
        P(("gx", "gy"), None),
        P(("gx", "gy")),
        P("gx", None, None),
        P("gx", None, None),
        P(None, ("gx", "gy")),
    )
    out_specs = P(None, None, ("gx", "gy"))
    return jax.shard_map(body, mesh=mesh, in_specs=in_specs, out_specs=out_specs, check_vma=False)
```

```python
import jax
import jax.numpy as jnp
from jax import lax
from jax.experimental import pallas as pl
from jax.experimental.pallas import tpu as pltpu
from jax.sharding import PartitionSpec as P


NODE_MIN = 16
LEVELS = 4
ITERS = 4
SLOT_CAP = 128
CHUNKS = 2
VMEM_LIMIT = 32 << 20
F32 = jnp.float32
BF16 = jnp.bfloat16
NN = (((1,), (0,)), ((), ()))
NT = (((1,), (1,)), ((), ()))


def split(value):
    high = value.astype(BF16)
    low = (value - high.astype(F32)).astype(BF16)
    return high, low


def mm(a, b, dims=NN):
    return lax.dot_general(a, b, dims, preferred_element_type=F32)


def pick(value, onehot, dims):
    high, low = split(value)
    return mm(high, onehot, dims) + mm(low, onehot, dims)


VM = pl.BlockSpec(memory_space=pltpu.VMEM)
FAR = pl.BlockSpec(memory_space=pltpu.HBM)
ANY = pl.BlockSpec(memory_space=pl.ANY)


def near(*values):
    return tuple(pltpu.with_memory_space_constraint(v, pltpu.VMEM) for v in values)


def call(kernel, outs, far=(), values=(), scratch=(), far_out=False, flops=0):
    if far_out:
        out_shape = tuple(jax.ShapeDtypeStruct(shape, kind) for shape, kind in outs)
    else:
        out_shape = tuple(pltpu.VMEM(shape, kind) for shape, kind in outs)
    return pl.pallas_call(
        kernel,
        out_shape=out_shape,
        in_specs=[FAR] * len(far) + [VM] * len(values),
        out_specs=tuple(ANY if far_out else VM for _ in outs),
        scratch_shapes=list(scratch),
        compiler_params=pltpu.CompilerParams(vmem_limit_bytes=VMEM_LIMIT),
        cost_estimate=pl.CostEstimate(flops=flops, transcendentals=0, bytes_accessed=1 << 20),
    )(*(pltpu.with_memory_space_constraint(v, pltpu.HBM) for v in far), *near(*values))


def take_share(operator, inverse, rows):
    width = operator.shape[1]

    part = rows // CHUNKS

    def kernel(op_ref, inv_ref, *rest):
        seat = lax.axis_index("gy")
        sems = rest[-1]

        def load(src):
            copies = [
                pltpu.make_async_copy(
                    src.at[pl.ds((seat // 2) * rows + c * part, part)], rest[c], sems.at[c]
                )
                for c in range(CHUNKS)
            ]
            for copy in copies:
                copy.start()
            for copy in copies:
                copy.wait()

        @pl.when(seat % 2 == 0)
        def _():
            load(inv_ref)

        @pl.when(seat % 2 != 0)
        def _():
            load(op_ref)

    return call(
        kernel,
        [((part, width), F32)] * CHUNKS,
        far=(operator, inverse),
        scratch=[pltpu.SemaphoreType.DMA((CHUNKS,))],
        flops=1 << 20,
    )


def pack_blocks(operator, inverse, mobility, nodes):
    half, quarter = nodes // 2, nodes // 4
    entries, seat_lanes = mobility.shape
    groups = -(-entries // 8)
    assert 2 * seat_lanes == nodes and groups <= 8

    def kernel(op_ref, inv_ref, mob_ref, mid_ref, small_ref, ext_ref, buf, sems):
        seat = lax.axis_index("gy")
        level = lax.axis_index("gx") % LEVELS

        def load(src):
            copies = [
                pltpu.make_async_copy(
                    src.at[pl.ds(c * nodes, half)], buf.at[pl.ds(c * half, half)], sems.at[c]
                )
                for c in range(4)
            ]
            for copy in copies:
                copy.start()
            for copy in copies:
                copy.wait()

        @pl.when(seat % 2 == 0)
        def _():
            load(inv_ref)

        @pl.when(seat % 2 != 0)
        def _():
            load(op_ref)

        lane = lax.broadcasted_iota(jnp.int32, (4 * half, nodes), 1)
        for pair in range(2):
            first = buf[:, pl.ds(2 * pair * nodes, nodes)]
            second = pltpu.roll(buf[:, pl.ds((2 * pair + 1) * nodes, nodes)], half, 1)
            mid_ref[:, pl.ds(pair * nodes, nodes)] = jnp.where(lane < half, first, second)
        count = jnp.left_shift(jnp.int32(NODE_MIN), level)
        lane = lax.broadcasted_iota(jnp.int32, (quarter, nodes), 1)
        row = lax.broadcasted_iota(jnp.int32, (quarter, nodes), 0)
        keep = ((lane % quarter) < count) & (row < count)
        for c in range(4):
            block = jnp.zeros((quarter, nodes), F32)
            for d in range(4):
                part = buf[pl.ds(c * half, quarter), pl.ds(d * nodes, nodes)]
                if d:
                    part = pltpu.roll(part, d * quarter, 1)
                block = jnp.where(lane // quarter == d, part, block)
            small_ref[pl.ds(c * quarter, quarter), :] = jnp.where(keep, block, 0.0)
        parts = []
        for g in range(8):
            size = max(0, min(8, entries - 8 * g))
            part = jnp.zeros((8, seat_lanes), F32)
            if size:
                part = mob_ref[pl.ds(8 * g, size), :]
                if size < 8:
                    part = jnp.concatenate([part, jnp.zeros((8 - size, seat_lanes), F32)], axis=0)
            parts.append(part)
        ext_ref[...] = jnp.concatenate(parts, axis=1)

    return call(
        kernel,
        [
            ((4 * half, 4 * half), F32),
            ((4 * quarter, 4 * quarter), F32),
            ((8, 8 * seat_lanes), F32),
        ],
        far=(operator, inverse),
        values=(mobility,),
        scratch=[pltpu.VMEM((4 * half, 4 * nodes), F32), pltpu.SemaphoreType.DMA((4,))],
        flops=1 << 20,
    )


def choose(own, got, source, extra=None):
    rows, width = own.shape
    more = () if extra is None else (extra,)

    def kernel(*refs):
        out_ref = refs[-1]
        gx = lax.axis_index("gx")
        for target, ref in [(source, refs[0])] + list(zip(got, refs[1:])):
            @pl.when(gx == target)
            def _(ref=ref):
                out_ref[pl.ds(0, rows), :] = ref[...]
        if more:
            out_ref[pl.ds(rows, extra.shape[0]), :] = refs[-2][...]

    height = rows + (extra.shape[0] if more else 0)
    return call(
        kernel, [((height, width), F32)], values=(own, *got.values(), *more), flops=1 << 20
    )[0]


def gather_low(mids, smalls):
    flat = [v for own, got, _ in mids for v in (own, *got.values())]
    side = mids[0][0].shape[0]
    lanes = smalls[0].shape[1]
    start_small = len(mids) * 2 * side
    height = start_small + len(smalls) * smalls[0].shape[0]

    def kernel(*refs):
        out_ref = refs[-1]
        gx = lax.axis_index("gx")
        at = 0
        for j, (_, got, source) in enumerate(mids):
            for target in [source] + list(got):
                ref = refs[at]
                at += 1

                @pl.when(gx == target)
                def _(ref=ref, j=j):
                    for h in range(2):
                        out_ref[pl.ds((2 * j + h) * side, side), :] = (
                            ref[:, pl.ds(h * lanes, lanes)]
                        )
        for k in range(len(smalls)):
            out_ref[pl.ds(start_small + k * lanes, lanes), :] = refs[at + k][...]

    return call(kernel, [((height, lanes), F32)], values=(*flat, *smalls), flops=1 << 20)[0]


def grade(buckets):
    small = [b for b in range(buckets) if b % LEVELS < LEVELS - 2]
    mid = [b for b in range(buckets) if b % LEVELS == LEVELS - 2]
    top = [b for b in range(buckets) if b % LEVELS == LEVELS - 1]
    return small, mid, top


def sort_fibers(bucket, attach, lengths, rhs, offsets, buckets, centres, nodes):
    fibers = bucket.shape[1]
    groups = grade(buckets)
    order = [b for group in groups for b in group]
    spans = [nodes // 4, nodes // 2, nodes]

    def kernel(bk_ref, at_ref, len_ref, rhs_ref, off_ref, oh_ref, s_ref, *rest):
        sorted_refs, aux_ref = rest[:3], rest[3]
        bk = bk_ref[...]
        ids = lax.broadcasted_iota(jnp.int32, (max(8, buckets), fibers), 0)
        mark = (ids == bk).astype(BF16)
        upper = (
            lax.broadcasted_iota(jnp.int32, (fibers, fibers), 0)
            < lax.broadcasted_iota(jnp.int32, (fibers, fibers), 1)
        ).astype(BF16)
        before = mm(mark, upper)
        place = jnp.sum(jnp.where(ids == bk, before, 0.0), axis=0, keepdims=True).astype(jnp.int32)
        slot = lax.broadcasted_iota(jnp.int32, (SLOT_CAP, fibers), 0)
        for k, b in enumerate(order):
            hot = (slot == place) & (bk == b)
            oh_ref[pl.ds(k * SLOT_CAP, SLOT_CAP), :] = hot.astype(BF16)
        onehot = oh_ref[...]
        centre = (
            lax.broadcasted_iota(jnp.int32, (centres, fibers), 0) == at_ref[...]
        ).astype(BF16)
        s_ref[...] = mm(onehot, centre, NT).astype(BF16)
        length = len_ref[...]
        row = lax.broadcasted_iota(jnp.int32, (8, fibers), 0)
        aux = jnp.where(row == 0, 0.3 / length, jnp.where(row == 1, length, 0.0))
        aux_ref[...] = pick(aux, onehot, NT)
        start = 0
        for group, span, ref in zip(groups, spans, sorted_refs):
            hot = oh_ref[pl.ds(start, len(group) * SLOT_CAP), :]
            start += len(group) * SLOT_CAP
            for c in range(7):
                src = rhs_ref[c, pl.ds(0, span), :] if c < 4 else off_ref[c - 4, pl.ds(0, span), :]
                ref[pl.ds(c * span, span), :] = pick(src, hot, NT)

    return call(
        kernel,
        [
            ((buckets * SLOT_CAP, fibers), BF16),
            ((buckets * SLOT_CAP, centres), BF16),
            *[
                ((7 * span, len(group) * SLOT_CAP), F32)
                for group, span in zip(groups, spans)
            ],
            ((8, buckets * SLOT_CAP), F32),
        ],
        values=(bucket, attach, lengths, rhs, offsets),
        flops=1 << 30,
    )


def product(matrix, vector):
    high, low = matrix
    v_high, v_low = split(vector)
    width = vector.shape[1]
    both = mm(high, jnp.concatenate([v_high, v_low], axis=1))
    return both[:, :width] + both[:, width:] + mm(low, v_high)


def couple(geometry, vector, n):
    u = [vector[c * n:(c + 1) * n] for c in range(4)]
    o = [geometry[c * n:(c + 1) * n] for c in range(3)]
    along = o[0] * u[0] + o[1] * u[1] + o[2] * u[2]
    pull = along + u[3]
    return 0.15 * jnp.concatenate([o[0] * pull, o[1] * pull, o[2] * pull, along], axis=0)


def sweeps(systems):
    vectors = [product(inverse, source) for inverse, _, source, _, _, _ in systems]
    for _ in range(ITERS):
        forces = [
            source - factor * product(stiffness, v) - couple(geometry, v, n)
            for v, (_, stiffness, source, geometry, factor, n) in zip(vectors, systems)
        ]
        vectors = [product(system[0], force) for force, system in zip(forces, systems)]
    return vectors


def wrench_rows(vector, geometry, length, n, count):
    u = [vector[c * n:(c + 1) * n] for c in range(3)]
    o = [geometry[c * n:(c + 1) * n] for c in range(3)]
    sums = [jnp.sum(v, axis=0, keepdims=True) for v in u]
    for a, b in ((1, 2), (2, 0), (0, 1)):
        sums.append(jnp.sum(o[a] * u[b] - o[b] * u[a], axis=0, keepdims=True))
    zero = jnp.zeros_like(sums[0])
    return (length / count) * jnp.concatenate(sums + [zero, zero], axis=0)


def solve_low(own, other, sorted_small, sorted_mid, aux, slots, buckets, nodes):
    small, mid, _ = grade(buckets)
    centres = slots.shape[1]
    half, quarter = nodes // 2, nodes // 4

    side = 4 * half
    start_small = len(mid) * 2 * side

    def mid_block(ref, j):
        parts = [ref[pl.ds((2 * j + h) * side, side), :] for h in range(2)]
        return jnp.concatenate(parts, axis=1)

    def kernel(own_ref, other_ref, ss_ref, sm_ref, aux_ref, slot_ref, xs_ref, xm_ref, t_ref):
        gx = lax.axis_index("gx")
        first = lax.axis_index("gy") % 2 == 0
        systems, lengths, counts = [], [], []
        for k, b in enumerate(small + mid):
            lanes = pl.ds(k * SLOT_CAP, SLOT_CAP)
            if k < len(small):
                index = lax.rem(b - gx + buckets, buckets)
                place = pl.ds(pl.multiple_of(start_small + index * nodes, nodes), nodes)
                mine, theirs = own_ref[place, :], other_ref[place, :]
                ref, here, n = ss_ref, lanes, quarter
            else:
                j = k - len(small)
                here = pl.ds(j * SLOT_CAP, SLOT_CAP)
                mine, theirs = mid_block(own_ref, j), mid_block(other_ref, j)
                ref, n = sm_ref, half
            systems.append(
                (
                    split(jnp.where(first, mine, theirs)),
                    split(jnp.where(first, theirs, mine)),
                    ref[pl.ds(0, 4 * n), here],
                    ref[pl.ds(4 * n, 3 * n), here],
                    aux_ref[pl.ds(0, 1), lanes],
                    n,
                )
            )
            lengths.append(aux_ref[pl.ds(1, 1), lanes])
            counts.append(float(NODE_MIN * 2 ** (b % LEVELS)))
        vectors = sweeps(systems)
        table = jnp.zeros((8, centres), F32)
        for k, vector in enumerate(vectors):
            _, _, _, geometry, _, n = systems[k]
            rows = wrench_rows(vector, geometry, lengths[k], n, counts[k])
            table = table + pick(rows, slot_ref[pl.ds(k * SLOT_CAP, SLOT_CAP), :], NN)
            if k < len(small):
                xs_ref[:, pl.ds(k * SLOT_CAP, SLOT_CAP)] = vector
            else:
                xm_ref[:, pl.ds((k - len(small)) * SLOT_CAP, SLOT_CAP)] = vector
        t_ref[...] = table

    return call(
        kernel,
        [
            ((4 * quarter, len(small) * SLOT_CAP), F32),
            ((4 * half, len(mid) * SLOT_CAP), F32),
            ((8, centres), F32),
        ],
        values=(own, other, sorted_small, sorted_mid, aux, slots),
        flops=1 << 30,
    )


def solve_top(pieces, top, aux, slots, table, buckets, nodes, rows):
    _, _, names = grade(buckets)
    n_low = buckets - len(names)
    width = LEVELS * nodes
    centres = slots.shape[1]
    shares = width // rows
    part = rows // CHUNKS
    flat = [p for chunks in pieces for pair in chunks for side in pair for p in side]

    def kernel(*refs):
        piece_refs = refs[:len(flat)]
        top_ref, aux_ref, slot_ref, tin_ref, x_ref, t_ref, high, low = refs[len(flat):]
        seat = lax.axis_index("gy")
        chip, core = seat // 2, seat % 2
        total = tin_ref[...]
        for k in range(len(names)):
            for i in range(CHUNKS * 2 * shares):
                c, side, m = i // (2 * shares), (i // shares) % 2, i % shares
                matrix = core if side == 0 else 1 - core
                h, l = split(piece_refs[k * CHUNKS * 2 * shares + i][pl.ds(0, part), :])
                start = jnp.bitwise_xor(chip, m) * rows + c * part
                place = pl.ds(pl.multiple_of(start, part), part)
                high[matrix, place, :] = h
                low[matrix, place, :] = l
            lanes = pl.ds(k * SLOT_CAP, SLOT_CAP)
            aux_lanes = pl.ds((n_low + k) * SLOT_CAP, SLOT_CAP)
            source = top_ref[pl.ds(0, width), lanes]
            geometry = top_ref[pl.ds(width, 3 * nodes), lanes]
            factor = aux_ref[pl.ds(0, 1), aux_lanes]
            length = aux_ref[pl.ds(1, 1), aux_lanes]
            (vector,) = sweeps(
                [((high[0], low[0]), (high[1], low[1]), source, geometry, factor, nodes)]
            )
            x_ref[:, lanes] = vector
            out = wrench_rows(vector, geometry, length, nodes, float(nodes))
            total = total + pick(out, slot_ref[aux_lanes, :], NN)
        t_ref[...] = total

    return call(
        kernel,
        [((width, len(names) * SLOT_CAP), F32), ((8, centres), F32)],
        values=(*flat, top, aux, slots, table),
        scratch=[
            pltpu.VMEM((2, width, width), BF16),
            pltpu.VMEM((2, width, width), BF16),
        ],
        flops=1 << 31,
    )


def unsort(parts, onehot, pieces, nodes, rows):
    fibers = onehot.shape[1]
    spans = [nodes // 4, nodes // 2, nodes]
    own, other = pieces
    chips = len(own)

    def kernel(*refs):
        part_refs, oh_ref = refs[:3], refs[3]
        own_refs, other_refs = refs[4:4 + chips], refs[4 + chips:4 + 2 * chips]
        out_ref, mob_ref = refs[4 + 2 * chips:]
        for c in range(4):
            total, start = None, 0
            for ref, span in zip(part_refs, spans):
                hot = oh_ref[pl.ds(start, ref.shape[1]), :]
                start += ref.shape[1]
                value = pick(ref[pl.ds(c * span, span), :], hot, NN)
                if total is not None:
                    low = total.shape[0]
                    value = jnp.concatenate([value[:low] + total, value[low:]], axis=0)
                total = value
            out_ref[c] = total
        seat = lax.axis_index("gy")
        chip, even = seat // 2, seat % 2 == 0
        lane = lax.broadcasted_iota(jnp.int32, (8, nodes), 1)
        half = nodes // 2
        for m in range(chips):
            place = pl.ds(pl.multiple_of(jnp.bitwise_xor(chip, m) * nodes, nodes), nodes)
            for g in range(mob_ref.shape[0] // 8):
                tile = pl.ds((g // 2) * nodes, nodes)
                mine = own_refs[m][pl.ds(rows, 8), tile]
                theirs = other_refs[m][pl.ds(rows, 8), tile]
                first = jnp.where(even, mine, theirs)
                second = jnp.where(even, theirs, mine)
                if g % 2 == 0:
                    second = pltpu.roll(second, half, 1)
                else:
                    first = pltpu.roll(first, half, 1)
                mob_ref[pl.ds(8 * g, 8), place] = jnp.where(lane < half, first, second)

    return call(
        kernel,
        [((4, nodes, fibers), F32), ((40, chips * nodes), F32)],
        values=(*parts, onehot, *own, *other),
        flops=1 << 28,
    )


def finish(tables, mobility, bucket, attach, offsets, solved, nodes):
    fibers = bucket.shape[1]
    centres = mobility.shape[1]

    def kernel(*refs):
        t_refs = refs[:len(tables)]
        mob_ref, bk_ref, at_ref, off_ref, sol_ref, out_ref, buf, sems = refs[len(tables):]
        copies = [pltpu.make_async_copy(sol_ref.at[3], out_ref.at[3], sems.at[3])]
        copies[0].start()
        table = t_refs[0][...]
        for t in t_refs[1:]:
            table = table + t[...]
        rows = []
        for k in range(6):
            part = mob_ref[pl.ds(6 * k, 6), :] * table[:6]
            rows.append(jnp.sum(part, axis=0, keepdims=True))
        zero = jnp.zeros_like(rows[0])
        motion = jnp.concatenate(rows + [zero, zero], axis=0)
        centre = (
            lax.broadcasted_iota(jnp.int32, (centres, fibers), 0) == at_ref[...]
        ).astype(BF16)
        moving = pick(motion, centre, NN)
        counts = jnp.left_shift(jnp.int32(NODE_MIN), bk_ref[...] % LEVELS)
        mask = lax.broadcasted_iota(jnp.int32, (nodes, fibers), 0) < counts
        u = [moving[k:k + 1] for k in range(3)]
        w = [moving[3 + k:4 + k] for k in range(3)]
        for k, (a, b) in enumerate(((1, 2), (2, 0), (0, 1))):
            rigid = u[k] + (w[a] * off_ref[b] - w[b] * off_ref[a])
            buf[k] = sol_ref[k] + jnp.where(mask, rigid, 0.0)
            copy = pltpu.make_async_copy(buf.at[k], out_ref.at[k], sems.at[k])
            copy.start()
            copies.append(copy)
        for copy in copies:
            copy.wait()

    return call(
        kernel,
        [((4, nodes, fibers), F32)],
        values=(*tables, mobility, bucket, attach, offsets, solved),
        scratch=[pltpu.VMEM((3, nodes, fibers), F32), pltpu.SemaphoreType.DMA((4,))],
        far_out=True,
        flops=1 << 24,
    )[0]


def body(rhs, offsets, lengths, bucket, attach, operator, inverse, mobility):
    nodes, fibers = rhs.shape[1], rhs.shape[2]
    buckets = lax.axis_size("gx")
    seats = lax.axis_size("gy")
    chips = seats // 2
    rows = LEVELS * nodes // chips
    centres = mobility.shape[1] * seats
    small, mid, top = grade(buckets)

    def hop(value, m):
        return lax.ppermute(value, "gy", [(i, i ^ m) for i in range(seats)])

    def spread(value, source):
        got = {}
        for target in range(buckets):
            if target != source:
                got[target] = lax.ppermute(value, "gx", [(source, target)])
        return got

    share_parts = take_share(operator[0], inverse[0], rows)
    sent = [[spread(part, source) for part in share_parts] for source in top]
    block_mid, block_small, extra = pack_blocks(
        operator[0], inverse[0], mobility, nodes
    )
    mids = [(block_mid, spread(block_mid, source), source) for source in mid]
    shares = []
    for k, source in enumerate(top):
        for c, part in enumerate(share_parts):
            shares.append(
                choose(part, sent[k][c], source, extra if k == c == 0 else None)
            )
    smalls = [block_small]
    for shift in range(1, buckets):
        smalls.append(lax.ppermute(block_small, "gx", [(s, (s - shift) % buckets) for s in small]))
    own_low = gather_low(mids, smalls)
    other_low = hop(own_low, 1)

    bucket_row = bucket.reshape(1, fibers)
    attach_row = attach.reshape(1, fibers)
    onehot, slots, sorted_small, sorted_mid, sorted_top, aux = sort_fibers(
        bucket_row, attach_row, lengths.reshape(1, fibers), rhs, offsets,
        buckets, centres, nodes,
    )

    pieces = []
    for i, mine in enumerate(shares):
        k, c = i // CHUNKS, i % CHUNKS
        own = [mine] + [hop(mine, 2 * m) for m in range(1, chips)]
        other = [hop(piece, 1) for piece in own]
        if c == 0:
            pieces.append([])
        pieces[k].append((own, other))

    x_small, x_mid, table_low = solve_low(
        own_low, other_low, sorted_small, sorted_mid, aux, slots, buckets, nodes
    )
    x_top, table = solve_top(pieces, sorted_top, aux, slots, table_low, buckets, nodes, rows)

    table = table + hop(table, 1)
    tables = [table] + [hop(table, 2 * m) for m in range(1, chips)]
    solved, mobility_all = unsort(
        (x_small, x_mid, x_top), onehot, pieces[0][0], nodes, rows // CHUNKS
    )
    return finish(tables, mobility_all, bucket_row, attach_row, offsets, solved, nodes)


def solution(mesh):
    in_specs = (
        P(None, None, ("gx", "gy")),
        P(None, None, ("gx", "gy")),
        P(("gx", "gy")),
        P(("gx", "gy"), None),
        P(("gx", "gy")),
        P("gx", None, None),
        P("gx", None, None),
        P(None, ("gx", "gy")),
    )
    out_specs = P(None, None, ("gx", "gy"))
    return jax.shard_map(body, mesh=mesh, in_specs=in_specs, out_specs=out_specs, check_vma=False)
```
